128 devices in a mesh: traj: 8 (over z, y_hi), lon: 16 (over y_lo, x, core).
Axes of the slice: x: 4, y: 4 (y_hi: 2, y_lo: 2; y = y_hi * 2 + y_lo), z: 4, core: 2. Of those that a mesh axis runs over, the one named last changes fastest.
Arguments:
- states: float32 [8, 78, 16, 2048], P('traj', None, None, 'lon')
- obs_index: int32 [8, 4096], P('traj', 'lon'), may hold values from 0 to 32767, as said below
- obs_values: float32 [8, 78, 4096], P('traj', None, 'lon'), may hold values from -8 to 8
- first_weight: bfloat16 [256, 2106], replicated, may hold values from -0.125 to 0.125
- first_bias: float32 [256], replicated, may hold values from -4 to 4
- second_weight: bfloat16 [234, 2304], replicated, may hold values from -0.125 to 0.125
Outputs:
- updated: float32 [8, 78, 16, 2048], P('traj', None, None, 'lon')
The draws below stay inside these ranges and needn't reach their ends.
Inputs may be any that keep to these rules, and one draw needn't show every extreme that they name: Entries k of obs_index[t] with k // 256 = j lie in longitude columns j * 128 to (j + 1) * 128 - 1; the cells of one state are distinct.
All inputs are finite; a program needn't handle non-finite values.
Results may differ from the reference program's by a relative error of at most 0.0028.
Values may be sent and summed in bfloat16 or wider, within the bound.
No kernel may reach another device: no remote copies, remote signals or barrier semaphores. Data moves between devices by JAX's collectives and lax.ppermute only.
A program may use at most 128 MiB of HBM per device.

```python
import jax
import jax.numpy as jnp
from jax import lax

VARS = 78
HIDDEN_W = 256
LAT = 16
LON_DEV = 128
NOBS = 256
STEPS = 2
STATES = 8
LON = 2048
NOBS_ALL = 4096


def draw_states(key, part):
    base_key, var_key = jax.random.split(jax.random.fold_in(key, 11))
    base = jax.random.normal(base_key, (STATES, VARS, LAT, LON), jnp.float32)
    var_scale = jnp.exp(jax.random.uniform(var_key, (VARS,), jnp.float32, jnp.log(0.3), jnp.log(3.0)))
    state_scale = 1.0 + 0.35 * jnp.arange(STATES, dtype=jnp.float32) / max(STATES - 1, 1)
    lon_scale = 1.0 + 0.35 * jnp.arange(LON, dtype=jnp.float32) / LON
    field = base * var_scale[None, :, None, None] * state_scale[:, None, None, None] * lon_scale[None, None, None, :]
    return 0.3 * field


def draw_obs_index(key, part):
    bands = LON // LON_DEV
    keys = jax.random.split(jax.random.fold_in(key, 23), STATES * bands)
    chosen = jax.vmap(lambda k: jax.random.permutation(k, LAT * LON_DEV)[:NOBS])(keys)
    chosen = chosen.reshape(STATES, bands, NOBS).astype(jnp.int32)
    band = jnp.arange(bands, dtype=jnp.int32)[None, :, None]
    row = chosen // LON_DEV
    column = chosen % LON_DEV
    cell = row * LON + band * LON_DEV + column
    return cell.reshape(STATES, bands * NOBS).astype(jnp.int32)


def levels(own_key, dims, cuts, least, top_value):
    gain, own = 1.0, jax.random.fold_in(own_key, 6)
    for axis_at, parts in cuts:
        draws = jnp.exp(jax.random.uniform(jax.random.fold_in(own, axis_at), (parts,), jnp.float32, least / len(cuts), top_value / len(cuts)))
        gain = gain * jnp.repeat(draws, dims[axis_at] // parts).reshape([-1 if axis == axis_at else 1 for axis in range(len(dims))])
    return gain


def centred(key, dims, width, bound, cuts=(), kind=jnp.bfloat16):
    level = levels(key, dims, cuts, -0.22, 0.18) if cuts else 1.0
    entries = jax.random.normal(key, dims, jnp.float32) * width * level
    return jnp.minimum(jnp.maximum(entries, -bound), bound).astype(kind)


def setup_inputs(seed: int = 0) -> dict:
    arg_keys = jax.random.split(jax.random.key(seed), 7)
    states = draw_states(jax.random.fold_in(arg_keys[6], 71), 0)
    obs_index = draw_obs_index(jax.random.fold_in(arg_keys[6], 71), 0)
    obs_values = centred(arg_keys[2], (STATES, VARS, NOBS_ALL), 1.5, 8.0, ((0, 8), (2, 16)), jnp.float32)
    first_weight = centred(arg_keys[3], (HIDDEN_W, 27 * VARS), (27 * VARS) ** -0.5, 0.125)
    first_bias = centred(arg_keys[4], (HIDDEN_W,), 0.7, 4.0, (), jnp.float32)
    second_weight = centred(arg_keys[5], (3 * VARS, 9 * HIDDEN_W), (9 * HIDDEN_W) ** -0.5, 0.125)
    return {"states": states, "obs_index": obs_index, "obs_values": obs_values, "first_weight": first_weight, "first_bias": first_bias, "second_weight": second_weight}


def make_patches(padded, rows, cols):
    pieces = [padded[:, a:a + rows, b:b + cols] for a in range(3) for b in range(3)]
    stacked = jnp.stack(pieces, 0)
    return stacked.reshape(stacked.shape[0] * stacked.shape[1], rows * cols)

def pad_field(field):
    wrapped = jnp.concatenate([field[:, :, -1:], field, field[:, :, :1]], 2)
    return jnp.pad(wrapped, ((0, 0), (1, 1), (0, 0)))

def network(window, first_weight, first_bias, second_weight):
    rows = window.shape[1]
    cols = window.shape[2]
    patches = make_patches(pad_field(window), rows, cols)
    hidden = jnp.dot(first_weight, patches, preferred_element_type=jnp.float32) + first_bias[:, None]
    hidden = jax.nn.silu(hidden).astype(jnp.bfloat16).reshape(-1, rows, cols)
    patches = make_patches(pad_field(hidden), rows, cols)
    return jnp.dot(second_weight, patches, preferred_element_type=jnp.float32).reshape(-1, rows, cols)

def reference(states, obs_index, obs_values, first_weight, first_bias, second_weight):
    nvar = states.shape[1]
    rows = states.shape[2]
    cols = states.shape[3]
    count = states.shape[0] * rows * cols
    x = states
    for step in range(STEPS):
        moment = lax.optimization_barrier(jnp.sum(x * x, axis=(0, 2, 3))) / count
        scale = 1.0 / jnp.sqrt(moment + 1e-06)
        normed = (x * scale[None, :, None, None]).astype(jnp.bfloat16)
        blank = jnp.zeros_like(normed[:1])
        before = jnp.concatenate([blank, normed[:-1]], 0)
        after = jnp.concatenate([normed[1:], blank], 0)
        windows = jnp.concatenate([before, normed, after], 1)
        contrib = lax.map(lambda w: network(w, first_weight, first_bias, second_weight), windows)
        zero_part = jnp.zeros_like(contrib[:1, :nvar])
        score = contrib[:, nvar:2 * nvar]
        score = score + jnp.concatenate([zero_part, contrib[:-1, 2 * nvar:]], 0)
        score = score + jnp.concatenate([contrib[1:, :nvar], zero_part], 0)
        flat = x.reshape(x.shape[0], nvar, rows * cols)

        def guide_one(field, index, values):
            seen = field[:, index]
            return jnp.zeros_like(field).at[:, index].add(values - seen)
        guide = jax.vmap(guide_one)(flat, obs_index, obs_values).reshape(x.shape)
        x = x + 0.5 * (score + guide)
    return x
```

```python
import functools

import jax
import jax.numpy as jnp
from jax import lax
from jax.experimental import pallas as pl
from jax.experimental.pallas import tpu as pltpu
from jax.sharding import Mesh
from jax.sharding import PartitionSpec as P

STEPS = 2
LON = ("lon_0", "lon_1", "lon_2")
TRAJ = ("traj_0", "traj_1")
ALL = TRAJ + LON
LANES = 128
F32 = jnp.float32
BF16 = jnp.bfloat16
VMEM = pl.BlockSpec(memory_space=pltpu.VMEM)


def call(kernel, outs, scratch, *args):
    return pl.pallas_call(
        kernel,
        out_shape=outs,
        in_specs=[VMEM] * len(args),
        out_specs=[VMEM] * len(outs),
        scratch_shapes=scratch,
        compiler_params=pltpu.CompilerParams(vmem_limit_bytes=48 * 2**20),
        name=kernel.func.__name__ if isinstance(kernel, functools.partial) else kernel.__name__,
    )(*args)


def iota(shape, dim):
    return lax.broadcasted_iota(jnp.int32, shape, dim)


def prepare_kernel(nvar, x_ref, index_ref, values_ref, send_ref, base_ref, sums_ref, xs, xf, vs):
    lines, cols = x_ref.shape
    rows = lines // nvar
    xs[...] = jnp.zeros_like(xs)
    xs[:lines, :] = x_ref[...]
    vpad = xs.shape[0] // rows
    for r in range(rows):
        picked = xs[pl.ds(r, vpad, stride=rows), :]
        picked = jnp.concatenate([picked, jnp.zeros((LANES - vpad, cols), F32)], 0)
        xf[pl.ds(r, cols, stride=rows), :] = picked.T
    vs[...] = jnp.zeros_like(vs)
    vs[:, :nvar] = values_ref[...]
    turned = vs[...]
    high = turned.astype(BF16)
    rest = turned - high.astype(F32)
    middle = rest.astype(BF16)
    low = (rest - middle.astype(F32)).astype(BF16)
    table = jnp.concatenate([high, middle, low, jnp.ones_like(high)], 1)
    index = index_ref[...]
    place = (index % LANES) * rows + index // (16 * LANES)
    chunk = 256
    nobs = index.shape[1]

    def one(i, acc):
        at = pl.ds(i * chunk, chunk)
        x = xf[at, :]
        cell = iota((chunk, nobs), 0) + i * chunk
        picks = jnp.where(cell == place, 1.0, 0.0).astype(BF16)
        found = jnp.dot(picks, table, preferred_element_type=F32)
        obs = (found[:, :LANES] + found[:, LANES : 2 * LANES]) + found[:, 2 * LANES : 3 * LANES]
        keep = 1.0 - 0.5 * found[:, 3 * LANES :]
        lane = iota((chunk, LANES), 1)
        coarse = x.astype(BF16).astype(F32)
        fine = pltpu.roll(x - coarse, nvar, 1)
        again = pltpu.roll(fine, nvar, 1)
        state = jnp.where(lane < nvar, coarse, fine)
        seen = jnp.where(lane < nvar, obs, jnp.where(lane == LANES - 1, keep, again))
        out = pl.ds(i * (chunk // rows), chunk // rows)
        send_ref[out, :rows] = state.astype(BF16).reshape(chunk // rows, rows, LANES)
        send_ref[out, rows:] = seen.astype(BF16).reshape(chunk // rows, rows, LANES)
        base_ref[out] = (keep * keep * x + (keep + 1.0) * 0.5 * obs).reshape(chunk // rows, rows, LANES)
        return acc + jnp.sum((x * x).reshape(chunk // 8, 8, LANES), 0)

    acc = lax.fori_loop(0, cols * rows // chunk, one, jnp.zeros((8, LANES), F32))
    sums_ref[...] = jnp.broadcast_to(jnp.sum(acc, 0, keepdims=True), sums_ref.shape)


def weights_kernel(nvar, w1_ref, w2_ref, w1t_ref, w2t_ref, pad, flat):
    hid = w1_ref.shape[1]
    win = 3 * nvar
    rest = jnp.zeros((hid, hid - win), F32)
    flat[...] = w1_ref[...].astype(F32)
    pad[...] = jnp.zeros_like(pad)
    for d in range(3):
        for b in range(3):
            for a in range(3):
                at = (3 * a + b) * win + d * nvar
                pad[a * nvar : (a + 1) * nvar, :] = flat[at : at + nvar, :]
            w1t_ref[pl.ds((3 * d + b) * hid, hid), :] = pad[...].astype(BF16)
    for b in range(3):
        turned = []
        for a in range(3):
            pad[:win, :] = w2_ref[:, (3 * a + b) * hid : (3 * a + b + 1) * hid].astype(F32)
            turned.append(pad[...].T)
        for d in range(3):
            parts = [t[:, (2 - d) * nvar : (3 - d) * nvar] for t in turned]
            block = jnp.concatenate(parts + [rest], 1)
            w2t_ref[pl.ds((3 * d + b) * hid, hid), :] = block.astype(BF16)


def assemble_kernel(reach, x_ref, left_ref, right_ref, out_ref):
    parts = out_ref.shape[0]
    cols = x_ref.shape[0]
    each = cols // parts
    for k in range(parts):
        first, last = k * each - reach, (k + 1) * each + reach
        lo, hi = max(first, 0), min(last, cols)
        out_ref[k, lo - first : hi - first] = x_ref[lo:hi]
        if first < 0:
            out_ref[k, :-first] = left_ref[...]
        if last > cols:
            out_ref[k, hi - first :] = right_ref[...]


def moved(value, by, edge):
    row = iota(value.shape, 0) % 16
    return jnp.where(row == edge, 0.0, pltpu.roll(value, by % value.shape[0], 0))


def convolutions(nvar, read, parts_ref, w1_ref, bias_ref, w2_ref, window, hidden, count, write):
    states, cols = window.shape[0] - 2, window.shape[1]
    rows = window.shape[2]
    inner = hidden.shape[1]
    outer = inner - 2
    total = jnp.sum(parts_ref[...], 0, keepdims=True)
    scale = 1.0 / jnp.sqrt(total / count + 1e-06)
    for edge in (0, states + 1):
        window[edge] = jnp.zeros(window.shape[1:], BF16)
        hidden[edge] = jnp.zeros(hidden.shape[1:], BF16)

    def fill(t, _):
        normed = read(t) * scale
        lane = iota(normed.shape, 1)
        mid = pltpu.roll(normed, nvar, 1)
        low = jnp.where(lane < nvar, moved(normed, 1, 0), mid)
        high = pltpu.roll(moved(normed, -1, 15), 2 * nvar - LANES, 1)
        high = jnp.where(lane < 2 * nvar - LANES, mid, high)
        window[t + 1] = jnp.concatenate([low, high], 1).astype(BF16).reshape(cols, rows, 2 * LANES)
        return 0

    lax.fori_loop(0, states, fill, 0)

    def first(t, _):
        patches = [
            window[t + d, b : b + inner].reshape(inner * rows, 2 * LANES) for d in range(3) for b in range(3)
        ]
        value = jnp.dot(jnp.concatenate(patches, 1), w1_ref[...], preferred_element_type=F32)
        value = 0.5 * (value + bias_ref[...])
        value = value * (1.0 + jnp.tanh(value))
        hidden[t + 1] = value.astype(BF16).reshape(inner, rows, value.shape[1])
        return 0

    lax.fori_loop(0, states, first, 0)

    def second(t, carry):
        patches = [
            hidden[t + d, b : b + outer].reshape(outer * rows, 2 * LANES) for d in range(3) for b in range(3)
        ]
        value = jnp.dot(jnp.concatenate(patches, 1), w2_ref[...], preferred_element_type=F32)
        low, high = value[:, :LANES], value[:, LANES:]
        lane = iota(low.shape, 1)
        mid = pltpu.roll(jnp.where(lane >= nvar, low, high), LANES - nvar, 1)
        end = pltpu.roll(high, 2 * LANES - 2 * nvar, 1)
        score = moved(low, 1, 0) + mid + moved(end, -1, 15)
        return write(t, jnp.where(lane < nvar, score, 0.0), carry)

    return lax.fori_loop(0, states, second, jnp.zeros((8, LANES), F32))


def first_step_kernel(nvar, count, s_ref, parts_ref, w1_ref, bias_ref, w2_ref, x_ref, d_ref, sums_ref, window, hidden):
    rows = s_ref.shape[2] // 2
    wide = window.shape[1]
    outer = x_ref.shape[1]
    core = d_ref.shape[1]
    skip = (outer - core) // 2
    ring = (wide - outer) // 2

    def read(t):
        state = s_ref[t, :, :rows].astype(F32).reshape(wide * rows, LANES)
        seen = s_ref[t, :, rows:].astype(F32).reshape(wide * rows, LANES)
        lane = iota(state.shape, 1)
        left = LANES - nvar
        fine = jnp.where(lane < left, pltpu.roll(state, left, 1), pltpu.roll(seen, 2 * left, 1))
        x = jnp.where(lane < nvar, state + fine, 0.0)
        mixed = (seen[:, LANES - 1 :] * x + 0.5 * seen).reshape(wide, rows, LANES)
        x_ref[t] = mixed[ring : ring + outer]
        return x

    def write(t, score, acc):
        mixed = x_ref[t].reshape(outer * rows, LANES)
        keep = s_ref[t, ring : ring + outer, rows:].astype(F32).reshape(outer * rows, LANES)[:, LANES - 1 :]
        half = 0.5 * score
        lane = iota(score.shape, 1)
        x = jnp.where(lane < nvar, mixed + half, 0.0)
        x_ref[t] = x.reshape(outer, rows, LANES)
        d_ref[t] = (keep * half).reshape(outer, rows, LANES)[skip : skip + core]
        own = x.reshape(outer, rows, LANES)[skip : skip + core]
        return acc + jnp.sum((own * own).reshape(core * rows // 8, 8, LANES), 0)

    acc = convolutions(nvar, read, parts_ref, w1_ref, bias_ref, w2_ref, window, hidden, count, write)
    sums_ref[...] = jnp.broadcast_to(jnp.sum(acc, 0, keepdims=True), sums_ref.shape)


def second_step_kernel(nvar, count, x_ref, d_ref, parts_ref, w1_ref, bias_ref, w2_ref, out_ref, window, hidden):
    wide, rows = x_ref.shape[1], x_ref.shape[2]
    core = d_ref.shape[1]

    def read(t):
        return x_ref[t].reshape(wide * rows, LANES)

    def write(t, score, acc):
        d = d_ref[t].reshape(core * rows, LANES) + 0.5 * score
        coarse = d.astype(BF16).astype(F32)
        lane = iota(d.shape, 1)
        d = jnp.where(lane < nvar, coarse, pltpu.roll(d - coarse, nvar, 1))
        out_ref[t] = d.astype(BF16).reshape(core, rows, LANES)
        return acc

    convolutions(nvar, read, parts_ref, w1_ref, bias_ref, w2_ref, window, hidden, count, write)


def finish_kernel(nvar, d_ref, base_ref, out_ref, both):
    cols, rows, _ = base_ref.shape
    d = d_ref[...].astype(F32).reshape(cols * rows, LANES)
    left = LANES - nvar
    fine = jnp.where(iota(d.shape, 1) < left, pltpu.roll(d, left, 1), 0.0)
    both[...] = base_ref[...].reshape(cols * rows, LANES) + d + fine
    for r in range(rows):
        turned = both[pl.ds(r, cols, stride=rows), :].T
        out_ref[pl.ds(r, nvar, stride=rows), :] = turned[:nvar]


def exchanged(rows, axes):
    return lax.all_to_all(rows[:, None, :], axes, 0, 0)[:, 0, :]


def body(states, obs_index, obs_values, first_weight, first_bias, second_weight):
    _, nvar, rows, cols = states.shape
    hid = first_weight.shape[0]
    parts = lax.axis_size(TRAJ)
    bands = lax.axis_size(LON)
    count = float(parts * bands * rows * cols)
    each = cols // parts
    vpad = -(-nvar // 8) * 8
    sds = jax.ShapeDtypeStruct
    everyone = sds((parts * bands, LANES), F32)
    band = (cols, rows, LANES)
    packed, base, sums = call(
        functools.partial(prepare_kernel, nvar),
        [sds((cols, 2 * rows, LANES), BF16), sds(band, F32), everyone],
        [
            pltpu.VMEM((vpad * rows, cols), F32),
            pltpu.VMEM((cols * rows, LANES), F32),
            pltpu.VMEM((obs_index.shape[1], LANES), F32),
        ],
        states.reshape(nvar * rows, cols),
        obs_index,
        obs_values[0].T,
    )
    wide = 2 * STEPS
    up = [(i, (i + 1) % bands) for i in range(bands)]
    down = [(j, i) for i, j in up]
    left = lax.ppermute(packed[cols - wide :], LON, up)
    right = lax.ppermute(packed[:wide], LON, down)
    w1, w2 = call(
        functools.partial(weights_kernel, nvar),
        [sds((9 * hid, hid), BF16), sds((9 * hid, hid), BF16)],
        [pltpu.VMEM((hid, hid), F32), pltpu.VMEM(first_weight.shape[::-1], F32)],
        first_weight.T,
        second_weight,
    )
    bias = first_bias[None]
    (sent,) = call(
        functools.partial(assemble_kernel, wide),
        [sds((parts, each + 2 * wide, 2 * rows, LANES), BF16)],
        [],
        packed,
        left,
        right,
    )
    got = lax.all_to_all(sent, TRAJ, 0, 0)
    x1, d1, sums1 = call(
        functools.partial(first_step_kernel, nvar, count),
        [sds((parts, each + 4, rows, LANES), F32), sds((parts, each, rows, LANES), F32), everyone],
        [pltpu.VMEM((parts + 2, each + 8, rows, hid), BF16), pltpu.VMEM((parts + 2, each + 6, rows, hid), BF16)],
        got,
        exchanged(sums, ALL),
        w1,
        bias,
        w2,
    )
    (d2,) = call(
        functools.partial(second_step_kernel, nvar, count),
        [sds((parts, each, rows, LANES), BF16)],
        [pltpu.VMEM((parts + 2, each + 4, rows, hid), BF16), pltpu.VMEM((parts + 2, each + 2, rows, hid), BF16)],
        x1,
        d1,
        exchanged(sums1, ALL),
        w1,
        bias,
        w2,
    )
    back = lax.all_to_all(d2, TRAJ, 0, 0)
    (out,) = call(
        functools.partial(finish_kernel, nvar),
        [sds((nvar * rows, cols), F32)],
        [pltpu.VMEM((cols * rows, LANES), F32)],
        back.reshape(cols, rows, LANES),
        base,
    )
    return out.reshape(states.shape)


def solution(mesh):
    torus = Mesh(
        mesh.devices.reshape(4, 2, 2, 4, 2), ("traj_0", "traj_1", "lon_0", "lon_1", "lon_2")
    )
    placed = (P(TRAJ, None, None, LON), P(TRAJ, LON), P(TRAJ, None, LON), P(), P(), P())
    return jax.shard_map(
        body, mesh=torus, in_specs=placed, out_specs=P(TRAJ, None, None, LON), check_vma=False
    )
```

```python
import functools

import jax
import jax.numpy as jnp
from jax import lax
from jax.experimental import pallas as pl
from jax.experimental.pallas import tpu as pltpu
from jax.sharding import Mesh
from jax.sharding import PartitionSpec as P

STEPS = 2
LON = ("lon_0", "lon_1", "lon_2")
TRAJ = ("traj_0", "traj_1")
ALL = TRAJ + LON
LANES = 128
F32 = jnp.float32
BF16 = jnp.bfloat16
VMEM = pl.BlockSpec(memory_space=pltpu.VMEM)


def call(kernel, outs, scratch, *args, far=0):
    return pl.pallas_call(
        kernel,
        out_shape=outs,
        in_specs=[pl.BlockSpec(memory_space=pltpu.HBM)] * far + [VMEM] * (len(args) - far),
        out_specs=[VMEM] * len(outs),
        scratch_shapes=scratch,
        compiler_params=pltpu.CompilerParams(vmem_limit_bytes=16 * 2**20),
        name=kernel.func.__name__ if isinstance(kernel, functools.partial) else kernel.__name__,
    )(*args)


def iota(shape, dim):
    return lax.broadcasted_iota(jnp.int32, shape, dim)


def fetch(nvar, x_ref, index_ref, values_ref, xs, xf, vs, index, values, sems):
    copies = [
        pltpu.make_async_copy(x_ref, xs.at[: x_ref.shape[0]], sems.at[0]),
        pltpu.make_async_copy(index_ref, index, sems.at[1]),
        pltpu.make_async_copy(values_ref, values, sems.at[2]),
    ]
    for copy in copies:
        copy.start()
    cols = xs.shape[1]
    rows = xf.shape[0] // cols
    vpad = xs.shape[0] // rows
    xs[nvar * rows :, :] = jnp.zeros((xs.shape[0] - nvar * rows, cols), F32)
    vs[...] = jnp.zeros_like(vs)
    for copy in copies:
        copy.wait()
    vs[:nvar, :] = values[:, 0, :]
    turned = vs[...].T
    high = turned.astype(BF16)
    rest = turned - high.astype(F32)
    middle = rest.astype(BF16)
    low = (rest - middle.astype(F32)).astype(BF16)
    table = jnp.concatenate([high, middle, low, jnp.ones_like(high)], 1)
    place = (index[...] % LANES) * rows + index[...] // (16 * LANES)
    for r in range(rows):
        picked = xs[pl.ds(r, vpad, stride=rows), :]
        picked = jnp.concatenate([picked, jnp.zeros((LANES - vpad, cols), F32)], 0)
        xf[pl.ds(r, cols, stride=rows), :] = picked.T

    def observed(start, size):
        cell = iota((size, index.shape[1]), 0) + start
        picks = jnp.where(cell == place, 1.0, 0.0).astype(BF16)
        found = jnp.dot(picks, table, preferred_element_type=F32)
        obs = (found[:, :LANES] + found[:, LANES : 2 * LANES]) + found[:, 2 * LANES : 3 * LANES]
        return obs, 1.0 - 0.5 * found[:, 3 * LANES :]

    return observed


CHUNK = 256


def prepare_kernel(nvar, x_ref, index_ref, values_ref, send_ref, sums_ref, xs, xf, *rest):
    observed = fetch(nvar, x_ref, index_ref, values_ref, xs, xf, *rest)
    rows = send_ref.shape[1] // 2
    each = CHUNK // rows
    acc = jnp.zeros((8, LANES), F32)
    for i in range(xf.shape[0] // CHUNK):
        x = xf[i * CHUNK : (i + 1) * CHUNK, :]
        obs, keep = observed(i * CHUNK, CHUNK)
        lane = iota(x.shape, 1)
        coarse = x.astype(BF16).astype(F32)
        fine = pltpu.roll(x - coarse, nvar, 1)
        again = pltpu.roll(fine, nvar, 1)
        state = jnp.where(lane < nvar, coarse, fine)
        seen = jnp.where(lane < nvar, obs, jnp.where(lane == LANES - 1, keep, again))
        send_ref[i * each : (i + 1) * each, :rows] = state.astype(BF16).reshape(each, rows, LANES)
        send_ref[i * each : (i + 1) * each, rows:] = seen.astype(BF16).reshape(each, rows, LANES)
        acc = acc + jnp.sum((x * x).reshape(CHUNK // 8, 8, LANES), 0)
    sums_ref[...] = jnp.broadcast_to(jnp.sum(acc, 0, keepdims=True), sums_ref.shape)


def base_kernel(nvar, x_ref, index_ref, values_ref, after_ref, base_ref, xs, xf, *rest):
    observed = fetch(nvar, x_ref, index_ref, values_ref, xs, xf, *rest)
    rows = base_ref.shape[1]
    each = CHUNK // rows
    for i in range(xf.shape[0] // CHUNK):
        x = xf[i * CHUNK : (i + 1) * CHUNK, :]
        obs, keep = observed(i * CHUNK, CHUNK)
        base = keep * keep * x + (keep + 1.0) * 0.5 * obs
        base_ref[i * each : (i + 1) * each] = base.reshape(each, rows, LANES)


def weights_kernel(nvar, w1_ref, w2_ref, w1t_ref, w2t_ref, pad, flat):
    hid = w1_ref.shape[1]
    win = 3 * nvar
    rest = jnp.zeros((hid, hid - win), F32)
    flat[...] = w1_ref[...].astype(F32)
    pad[...] = jnp.zeros_like(pad)
    for d in range(3):
        for b in range(3):
            for a in range(3):
                at = (3 * a + b) * win + d * nvar
                pad[a * nvar : (a + 1) * nvar, :] = flat[at : at + nvar, :]
            w1t_ref[pl.ds((3 * d + b) * hid, hid), :] = pad[...].astype(BF16)
    for b in range(3):
        turned = []
        for a in range(3):
            pad[:win, :] = w2_ref[:, (3 * a + b) * hid : (3 * a + b + 1) * hid].astype(F32)
            turned.append(pad[...].T)
        for d in range(3):
            parts = [t[:, (2 - d) * nvar : (3 - d) * nvar] for t in turned]
            block = jnp.concatenate(parts + [rest], 1)
            w2t_ref[pl.ds((3 * d + b) * hid, hid), :] = block.astype(BF16)


def assemble_kernel(reach, x_ref, left_ref, right_ref, moments_ref, out_ref, done_ref):
    parts = out_ref.shape[0]
    cols = x_ref.shape[0]
    rows = x_ref.shape[1] // 2
    each = cols // parts
    total = jnp.broadcast_to(jnp.sum(moments_ref[...], 0, keepdims=True), (rows, LANES))
    high = total.astype(BF16).astype(F32)
    middle = (total - high).astype(BF16).astype(F32)
    row = iota(total.shape, 0)
    total = jnp.where(row == 0, high, jnp.where(row == 1, middle, jnp.where(row == 2, total - high - middle, 0.0)))
    total = total.astype(BF16)

    def fill(k, reach, half, to, skip):
        first, last = k * each - reach, (k + 1) * each + reach
        lo, hi = max(first, 0), min(last, cols)
        half = slice(half * rows, (half + 1) * rows)
        out_ref[k, to + lo - first : to + hi - first] = x_ref[lo:hi, half]
        if first < 0:
            out_ref[k, to : to - first] = left_ref[skip:, half]
        if last > cols:
            out_ref[k, to + hi - first : to + last - first] = right_ref[:reach, half]

    for k in range(parts):
        fill(k, reach, 0, 0, 0)
        fill(k, reach // 2, 1, each + 2 * reach, reach - reach // 2)
        out_ref[k, 2 * each + 3 * reach] = total
    done_ref[...] = moments_ref[:8, :]


def moved(value, by, edge):
    row = iota(value.shape, 0) % 16
    return jnp.where(row == edge, 0.0, pltpu.roll(value, by % value.shape[0], 0))


def convolutions(nvar, read, total, w2_far, w1_ref, bias_ref, window, hidden, w2_ref, sem, count, write):
    copy = pltpu.make_async_copy(w2_far, w2_ref, sem)
    copy.start()
    states, cols = window.shape[0] - 2, window.shape[1]
    rows = window.shape[2]
    inner = hidden.shape[1]
    outer = inner - 2
    scale = 1.0 / jnp.sqrt(total / count + 1e-06)
    for edge in (0, states + 1):
        window[edge] = jnp.zeros(window.shape[1:], BF16)
        hidden[edge] = jnp.zeros(hidden.shape[1:], BF16)

    def fill(t, _):
        normed = read(t) * scale
        lane = iota(normed.shape, 1)
        mid = pltpu.roll(normed, nvar, 1)
        low = jnp.where(lane < nvar, moved(normed, 1, 0), mid)
        high = pltpu.roll(moved(normed, -1, 15), 2 * nvar - LANES, 1)
        high = jnp.where(lane < 2 * nvar - LANES, mid, high)
        window[t + 1] = jnp.concatenate([low, high], 1).astype(BF16).reshape(cols, rows, 2 * LANES)
        return 0

    def first(t, _):
        patches = [
            window[t + d, b : b + inner].reshape(inner * rows, 2 * LANES) for d in range(3) for b in range(3)
        ]
        value = jnp.dot(jnp.concatenate(patches, 1), w1_ref[...], preferred_element_type=F32)
        value = 0.5 * (value + bias_ref[...])
        value = value * (1.0 + jnp.tanh(value))
        hidden[t + 1] = value.astype(BF16).reshape(inner, rows, value.shape[1])
        return 0

    def second(t, carry):
        patches = [
            hidden[t + d, b : b + outer].reshape(outer * rows, 2 * LANES) for d in range(3) for b in range(3)
        ]
        value = jnp.dot(jnp.concatenate(patches, 1), w2_ref[...], preferred_element_type=F32)
        low, high = value[:, :LANES], value[:, LANES:]
        lane = iota(low.shape, 1)
        mid = pltpu.roll(jnp.where(lane >= nvar, low, high), LANES - nvar, 1)
        end = pltpu.roll(high, 2 * LANES - 2 * nvar, 1)
        score = moved(low, 1, 0) + mid + moved(end, -1, 15)
        return write(t, jnp.where(lane < nvar, score, 0.0), carry)

    carry = jnp.zeros((8, LANES), F32)
    for t in range(states + 2):
        if t < states:
            fill(t, 0)
        if 1 <= t <= states:
            first(t - 1, 0)
        if t == 2:
            copy.wait()
        if t >= 2:
            carry = second(t - 2, carry)
    return carry


def first_step_kernel(nvar, count, w2_ref, s_ref, w1_ref, bias_ref, x_ref, d_ref, sums_ref, window, hidden, w2, sem):
    rows = s_ref.shape[2]
    wide = window.shape[1]
    outer = x_ref.shape[1]
    core = d_ref.shape[1]
    skip = (outer - core) // 2
    ring = (wide - outer) // 2

    def read(t):
        state = s_ref[t, :wide].astype(F32).reshape(wide * rows, LANES)
        seen = s_ref[t, wide : wide + outer].astype(F32).reshape(outer * rows, LANES)
        lane = iota(state.shape, 1)
        left = LANES - nvar
        none = jnp.zeros((ring * rows, LANES), F32)
        rest = jnp.concatenate([none, pltpu.roll(seen, 2 * left, 1), none], 0)
        fine = jnp.where(lane < left, pltpu.roll(state, left, 1), rest)
        x = jnp.where(lane < nvar, state + fine, 0.0)
        mixed = seen[:, LANES - 1 :] * x[ring * rows : (ring + outer) * rows] + 0.5 * seen
        x_ref[t] = mixed.reshape(outer, rows, LANES)
        return x

    def write(t, score, acc):
        mixed = x_ref[t].reshape(outer * rows, LANES)
        keep = s_ref[t, wide : wide + outer].astype(F32).reshape(outer * rows, LANES)[:, LANES - 1 :]
        half = 0.5 * score
        lane = iota(score.shape, 1)
        x = jnp.where(lane < nvar, mixed + half, 0.0)
        x_ref[t] = x.reshape(outer, rows, LANES)
        d_ref[t] = (keep * half).reshape(outer, rows, LANES)[skip : skip + core]
        own = x.reshape(outer, rows, LANES)[skip : skip + core]
        return acc + jnp.sum((own * own).reshape(core * rows // 8, 8, LANES), 0)

    total = jnp.sum(s_ref[:, wide + outer].astype(F32).reshape(-1, LANES), 0, keepdims=True)
    acc = convolutions(nvar, read, total, w2_ref, w1_ref, bias_ref, window, hidden, w2, sem, count, write)
    sums_ref[...] = jnp.broadcast_to(jnp.sum(acc, 0, keepdims=True), sums_ref.shape)


def second_step_kernel(nvar, count, w2_ref, x_ref, d_ref, parts_ref, w1_ref, bias_ref, out_ref, window, hidden, w2, sem):
    wide, rows = x_ref.shape[1], x_ref.shape[2]
    core = d_ref.shape[1]

    def read(t):
        return x_ref[t].reshape(wide * rows, LANES)

    def write(t, score, acc):
        d = d_ref[t].reshape(core * rows, LANES) + 0.5 * score
        coarse = d.astype(BF16).astype(F32)
        lane = iota(d.shape, 1)
        d = jnp.where(lane < nvar, coarse, pltpu.roll(d - coarse, nvar, 1))
        out_ref[t] = d.astype(BF16).reshape(core, rows, LANES)
        return acc

    total = jnp.sum(parts_ref[...], 0, keepdims=True)
    convolutions(nvar, read, total, w2_ref, w1_ref, bias_ref, window, hidden, w2, sem, count, write)


def finish_kernel(nvar, d_ref, base_ref, out_ref, both):
    cols, rows, _ = base_ref.shape
    d = d_ref[...].astype(F32).reshape(cols * rows, LANES)
    left = LANES - nvar
    fine = jnp.where(iota(d.shape, 1) < left, pltpu.roll(d, left, 1), 0.0)
    both[...] = base_ref[...].reshape(cols * rows, LANES) + d + fine
    for r in range(rows):
        turned = both[pl.ds(r, cols, stride=rows), :].T
        out_ref[pl.ds(r, nvar, stride=rows), :] = turned[:nvar]


def exchanged(rows, axes):
    return lax.all_to_all(rows[:, None, :], axes, 0, 0)[:, 0, :]


def body(states, obs_index, obs_values, first_weight, first_bias, second_weight):
    _, nvar, rows, cols = states.shape
    hid = first_weight.shape[0]
    parts = lax.axis_size(TRAJ)
    bands = lax.axis_size(LON)
    count = float(parts * bands * rows * cols)
    each = cols // parts
    vpad = -(-nvar // 8) * 8
    sds = jax.ShapeDtypeStruct
    everyone = sds((parts * bands, LANES), F32)
    band = (cols, rows, LANES)
    source = (states.reshape(nvar * rows, cols), obs_index, obs_values.transpose(1, 0, 2))
    source = [pltpu.with_memory_space_constraint(value, pltpu.HBM) for value in source]
    scratch = [
        pltpu.VMEM((vpad * rows, cols), F32),
        pltpu.VMEM((cols * rows, LANES), F32),
        pltpu.VMEM((LANES, obs_index.shape[1]), F32),
        pltpu.VMEM(obs_index.shape, jnp.int32),
        pltpu.VMEM((nvar, 1, obs_index.shape[1]), F32),
        pltpu.SemaphoreType.DMA((3,)),
    ]
    packed, sums = call(
        functools.partial(prepare_kernel, nvar),
        [sds((cols, 2 * rows, LANES), BF16), sds((bands, LANES), F32)],
        scratch,
        *source,
        far=3,
    )
    wide = 2 * STEPS
    up = [(i, (i + 1) % bands) for i in range(bands)]
    down = [(j, i) for i, j in up]
    left = lax.ppermute(packed[cols - wide :], LON, up)
    right = lax.ppermute(packed[:wide], LON, down)
    w1, w2 = call(
        functools.partial(weights_kernel, nvar),
        [sds((9 * hid, hid), BF16), sds((9 * hid, hid), BF16)],
        [pltpu.VMEM((hid, hid), F32), pltpu.VMEM(first_weight.shape[::-1], F32)],
        first_weight.T,
        second_weight,
    )
    bias = first_bias[None]
    sent, done = call(
        functools.partial(assemble_kernel, wide),
        [sds((parts, 2 * each + 3 * wide + 1, rows, LANES), BF16), sds((8, LANES), F32)],
        [],
        packed,
        left,
        right,
        exchanged(sums, LON),
    )
    got = lax.all_to_all(sent, TRAJ, 0, 0)
    (base,) = call(functools.partial(base_kernel, nvar), [sds(band, F32)], scratch, *source, done, far=4)
    w2 = pltpu.with_memory_space_constraint(w2, pltpu.HBM)

    def buffers(cols):
        return [
            pltpu.VMEM((parts + 2, cols, rows, hid), BF16),
            pltpu.VMEM((parts + 2, cols - 2, rows, hid), BF16),
            pltpu.VMEM(w2.shape, BF16),
            pltpu.SemaphoreType.DMA(()),
        ]

    x1, d1, sums1 = call(
        functools.partial(first_step_kernel, nvar, count),
        [sds((parts, each + 4, rows, LANES), F32), sds((parts, each, rows, LANES), F32), everyone],
        buffers(each + 8),
        w2,
        got,
        w1,
        bias,
        far=1,
    )
    (d2,) = call(
        functools.partial(second_step_kernel, nvar, count),
        [sds((parts, each, rows, LANES), BF16)],
        buffers(each + 4),
        w2,
        x1,
        d1,
        exchanged(sums1, ALL),
        w1,
        bias,
        far=1,
    )
    back = lax.all_to_all(d2, TRAJ, 0, 0)
    (out,) = call(
        functools.partial(finish_kernel, nvar),
        [sds((nvar * rows, cols), F32)],
        [pltpu.VMEM((cols * rows, LANES), F32)],
        back.reshape(cols, rows, LANES),
        base,
    )
    return out.reshape(states.shape)


def solution(mesh):
    torus = Mesh(
        mesh.devices.reshape(4, 2, 2, 4, 2), ("traj_0", "traj_1", "lon_0", "lon_1", "lon_2")
    )
    placed = (P(TRAJ, None, None, LON), P(TRAJ, LON), P(TRAJ, None, LON), P(), P(), P())
    return jax.shard_map(
        body, mesh=torus, in_specs=placed, out_specs=P(TRAJ, None, None, LON), check_vma=False
    )
```

```python
import functools

import jax
import jax.numpy as jnp
from jax import lax
from jax.experimental import pallas as pl
from jax.experimental.pallas import tpu as pltpu
from jax.sharding import Mesh
from jax.sharding import PartitionSpec as P

STEPS = 2
LON = ("lon_0", "lon_1", "lon_2")
TRAJ = ("traj_0", "traj_1")
ALL = TRAJ + LON
LANES = 128
F32 = jnp.float32
BF16 = jnp.bfloat16
VMEM = pl.BlockSpec(memory_space=pltpu.VMEM)


def call(kernel, outs, scratch, *args, far=0):
    return pl.pallas_call(
        kernel,
        out_shape=outs,
        in_specs=[pl.BlockSpec(memory_space=pltpu.HBM)] * far + [VMEM] * (len(args) - far),
        out_specs=[VMEM] * len(outs),
        scratch_shapes=scratch,
        compiler_params=pltpu.CompilerParams(vmem_limit_bytes=16 * 2**20),
        name=kernel.func.__name__ if isinstance(kernel, functools.partial) else kernel.__name__,
    )(*args)


def iota(shape, dim):
    return lax.broadcasted_iota(jnp.int32, shape, dim)


def fetch(nvar, x_ref, index_ref, values_ref, xs, xf, vs, index, values, sems):
    copies = [
        pltpu.make_async_copy(x_ref, xs.at[: x_ref.shape[0]], sems.at[0]),
        pltpu.make_async_copy(index_ref, index, sems.at[1]),
        pltpu.make_async_copy(values_ref, values, sems.at[2]),
    ]
    for copy in copies:
        copy.start()
    cols = xs.shape[1]
    rows = xf.shape[0] // cols
    vpad = xs.shape[0] // rows
    xs[nvar * rows :, :] = jnp.zeros((xs.shape[0] - nvar * rows, cols), F32)
    vs[...] = jnp.zeros_like(vs)
    for copy in copies:
        copy.wait()
    vs[:nvar, :] = values[:, 0, :]
    turned = vs[...].T
    high = turned.astype(BF16)
    rest = turned - high.astype(F32)
    middle = rest.astype(BF16)
    low = (rest - middle.astype(F32)).astype(BF16)
    table = jnp.concatenate([high, middle, low, jnp.ones_like(high)], 1)
    place = (index[...] % LANES) * rows + index[...] // (16 * LANES)
    for r in range(rows):
        picked = xs[pl.ds(r, vpad, stride=rows), :]
        picked = jnp.concatenate([picked, jnp.zeros((LANES - vpad, cols), F32)], 0)
        xf[pl.ds(r, cols, stride=rows), :] = picked.T

    def observed(start, size):
        cell = iota((size, index.shape[1]), 0) + start
        picks = jnp.where(cell == place, 1.0, 0.0).astype(BF16)
        found = jnp.dot(picks, table, preferred_element_type=F32)
        obs = (found[:, :LANES] + found[:, LANES : 2 * LANES]) + found[:, 2 * LANES : 3 * LANES]
        return obs, 1.0 - 0.5 * found[:, 3 * LANES :]

    return observed


CHUNK = 256


def prepare_kernel(nvar, x_ref, index_ref, values_ref, send_ref, sums_ref, xs, xf, *rest):
    observed = fetch(nvar, x_ref, index_ref, values_ref, xs, xf, *rest)
    rows = send_ref.shape[1] // 2
    each = CHUNK // rows
    acc = jnp.zeros((8, LANES), F32)
    for i in range(xf.shape[0] // CHUNK):
        x = xf[i * CHUNK : (i + 1) * CHUNK, :]
        obs, keep = observed(i * CHUNK, CHUNK)
        lane = iota(x.shape, 1)
        coarse = x.astype(BF16).astype(F32)
        fine = pltpu.roll(x - coarse, nvar, 1)
        again = pltpu.roll(fine, nvar, 1)
        state = jnp.where(lane < nvar, coarse, fine)
        seen = jnp.where(lane < nvar, obs, jnp.where(lane == LANES - 1, keep, again))
        send_ref[i * each : (i + 1) * each, :rows] = state.astype(BF16).reshape(each, rows, LANES)
        send_ref[i * each : (i + 1) * each, rows:] = seen.astype(BF16).reshape(each, rows, LANES)
        acc = acc + jnp.sum((x * x).reshape(CHUNK // 8, 8, LANES), 0)
    sums_ref[...] = jnp.broadcast_to(jnp.sum(acc, 0, keepdims=True), sums_ref.shape)


def base_kernel(nvar, x_ref, index_ref, values_ref, after_ref, base_ref, xs, xf, *rest):
    observed = fetch(nvar, x_ref, index_ref, values_ref, xs, xf, *rest)
    rows = base_ref.shape[1]
    each = CHUNK // rows
    for i in range(xf.shape[0] // CHUNK):
        x = xf[i * CHUNK : (i + 1) * CHUNK, :]
        obs, keep = observed(i * CHUNK, CHUNK)
        base = keep * keep * x + (keep + 1.0) * 0.5 * obs
        base_ref[i * each : (i + 1) * each] = base.reshape(each, rows, LANES)


def weights_kernel(nvar, w1_ref, w2_ref, out_ref, pad, flat):
    hid = w1_ref.shape[1]
    win = 3 * nvar
    rest = jnp.zeros((hid, hid - win), F32)
    flat[...] = w1_ref[...].astype(F32)
    pad[...] = jnp.zeros_like(pad)
    for d in range(3):
        for b in range(3):
            for a in range(3):
                at = (3 * a + b) * win + d * nvar
                pad[a * nvar : (a + 1) * nvar, :] = flat[at : at + nvar, :]
            out_ref[0, (3 * d + b) * hid : (3 * d + b + 1) * hid, :] = pad[...].astype(BF16)
    for b in range(3):
        turned = []
        for a in range(3):
            pad[:win, :] = w2_ref[:, (3 * a + b) * hid : (3 * a + b + 1) * hid].astype(F32)
            turned.append(pad[...].T)
        for d in range(3):
            parts = [t[:, (2 - d) * nvar : (3 - d) * nvar] for t in turned]
            block = jnp.concatenate(parts + [rest], 1)
            out_ref[1, (3 * d + b) * hid : (3 * d + b + 1) * hid, :] = block.astype(BF16)


def assemble_kernel(reach, x_ref, left_ref, right_ref, moments_ref, out_ref, done_ref):
    parts = out_ref.shape[0]
    cols = x_ref.shape[0]
    rows = x_ref.shape[1] // 2
    each = cols // parts
    total = jnp.broadcast_to(jnp.sum(moments_ref[...], 0, keepdims=True), (rows, LANES))
    high = total.astype(BF16).astype(F32)
    middle = (total - high).astype(BF16).astype(F32)
    row = iota(total.shape, 0)
    total = jnp.where(row == 0, high, jnp.where(row == 1, middle, jnp.where(row == 2, total - high - middle, 0.0)))
    total = total.astype(BF16)

    def fill(k, reach, half, to, skip):
        first, last = k * each - reach, (k + 1) * each + reach
        lo, hi = max(first, 0), min(last, cols)
        half = slice(half * rows, (half + 1) * rows)
        out_ref[k, to + lo - first : to + hi - first] = x_ref[lo:hi, half]
        if first < 0:
            out_ref[k, to : to - first] = left_ref[skip:, half]
        if last > cols:
            out_ref[k, to + hi - first : to + last - first] = right_ref[:reach, half]

    for k in range(parts):
        fill(k, reach, 0, 0, 0)
        fill(k, reach // 2, 1, each + 2 * reach, reach - reach // 2)
        out_ref[k, 2 * each + 3 * reach] = total
    done_ref[...] = moments_ref[:8, :]


def moved(value, by, edge):
    row = iota(value.shape, 0) % 16
    return jnp.where(row == edge, 0.0, pltpu.roll(value, by % value.shape[0], 0))


def convolutions(nvar, read, total, weights_ref, bias_ref, window, hidden, count, write):
    states, cols = window.shape[0] - 2, window.shape[1]
    rows = window.shape[2]
    inner = hidden.shape[1]
    outer = inner - 2
    scale = 1.0 / jnp.sqrt(total / count + 1e-06)
    for edge in (0, states + 1):
        window[edge] = jnp.zeros(window.shape[1:], BF16)
        hidden[edge] = jnp.zeros(hidden.shape[1:], BF16)

    def fill(t, _):
        normed = read(t) * scale
        lane = iota(normed.shape, 1)
        mid = pltpu.roll(normed, nvar, 1)
        low = jnp.where(lane < nvar, moved(normed, 1, 0), mid)
        high = pltpu.roll(moved(normed, -1, 15), 2 * nvar - LANES, 1)
        high = jnp.where(lane < 2 * nvar - LANES, mid, high)
        window[t + 1] = jnp.concatenate([low, high], 1).astype(BF16).reshape(cols, rows, 2 * LANES)
        return 0

    def first(t, _):
        patches = [
            window[t + d, b : b + inner].reshape(inner * rows, 2 * LANES) for d in range(3) for b in range(3)
        ]
        value = jnp.dot(jnp.concatenate(patches, 1), weights_ref[0], preferred_element_type=F32)
        value = 0.5 * (value + bias_ref[...])
        value = value * (1.0 + jnp.tanh(value))
        hidden[t + 1] = value.astype(BF16).reshape(inner, rows, value.shape[1])
        return 0

    def second(t, carry):
        patches = [
            hidden[t + d, b : b + outer].reshape(outer * rows, 2 * LANES) for d in range(3) for b in range(3)
        ]
        value = jnp.dot(jnp.concatenate(patches, 1), weights_ref[1], preferred_element_type=F32)
        low, high = value[:, :LANES], value[:, LANES:]
        lane = iota(low.shape, 1)
        mid = pltpu.roll(jnp.where(lane >= nvar, low, high), LANES - nvar, 1)
        end = pltpu.roll(high, 2 * LANES - 2 * nvar, 1)
        score = moved(low, 1, 0) + mid + moved(end, -1, 15)
        return write(t, jnp.where(lane < nvar, score, 0.0), carry)

    carry = jnp.zeros((8, LANES), F32)
    for t in range(states + 2):
        if t < states:
            fill(t, 0)
        if 1 <= t <= states:
            first(t - 1, 0)
        if t >= 2:
            carry = second(t - 2, carry)
    return carry


def first_step_kernel(
    nvar, count, _, far_ref, weights_ref, bias_ref, x_ref, d_ref, sums_ref, window, hidden, s_ref, moments, sems
):
    rows = s_ref.shape[2]
    states = s_ref.shape[0]
    copies = [pltpu.make_async_copy(far_ref.at[:, s_ref.shape[1]], moments, sems.at[states])]
    for t in range(states):
        copies.append(pltpu.make_async_copy(far_ref.at[t, : s_ref.shape[1]], s_ref.at[t], sems.at[t]))
    for copy in copies:
        copy.start()
    wide = window.shape[1]
    outer = x_ref.shape[1]
    core = d_ref.shape[1]
    skip = (outer - core) // 2
    ring = (wide - outer) // 2

    def read(t):
        for copy in copies[2:] if t == 1 else copies[1:2] if t == 0 else ():
            copy.wait()
        state = s_ref[t, :wide].astype(F32).reshape(wide * rows, LANES)
        seen = s_ref[t, wide : wide + outer].astype(F32).reshape(outer * rows, LANES)
        lane = iota(state.shape, 1)
        left = LANES - nvar
        none = jnp.zeros((ring * rows, LANES), F32)
        rest = jnp.concatenate([none, pltpu.roll(seen, 2 * left, 1), none], 0)
        fine = jnp.where(lane < left, pltpu.roll(state, left, 1), rest)
        x = jnp.where(lane < nvar, state + fine, 0.0)
        mixed = seen[:, LANES - 1 :] * x[ring * rows : (ring + outer) * rows] + 0.5 * seen
        x_ref[t] = mixed.reshape(outer, rows, LANES)
        return x

    def write(t, score, acc):
        mixed = x_ref[t].reshape(outer * rows, LANES)
        keep = s_ref[t, wide : wide + outer].astype(F32).reshape(outer * rows, LANES)[:, LANES - 1 :]
        half = 0.5 * score
        lane = iota(score.shape, 1)
        x = jnp.where(lane < nvar, mixed + half, 0.0)
        x_ref[t] = x.reshape(outer, rows, LANES)
        d_ref[t] = (keep * half).reshape(outer, rows, LANES)[skip : skip + core]
        own = x.reshape(outer, rows, LANES)[skip : skip + core]
        return acc + jnp.sum((own * own).reshape(core * rows // 8, 8, LANES), 0)

    copies[0].wait()
    total = jnp.sum(moments[...].astype(F32).reshape(-1, LANES), 0, keepdims=True)
    acc = convolutions(nvar, read, total, weights_ref, bias_ref, window, hidden, count, write)
    sums_ref[...] = jnp.broadcast_to(jnp.sum(acc, 0, keepdims=True), sums_ref.shape)


def second_step_kernel(nvar, count, x_ref, d_ref, parts_ref, weights_ref, bias_ref, out_ref, window, hidden):
    wide, rows = x_ref.shape[1], x_ref.shape[2]
    core = d_ref.shape[1]

    def read(t):
        return x_ref[t].reshape(wide * rows, LANES)

    def write(t, score, acc):
        d = d_ref[t].reshape(core * rows, LANES) + 0.5 * score
        coarse = d.astype(BF16).astype(F32)
        lane = iota(d.shape, 1)
        d = jnp.where(lane < nvar, coarse, pltpu.roll(d - coarse, nvar, 1))
        out_ref[t] = d.astype(BF16).reshape(core, rows, LANES)
        return acc

    total = jnp.sum(parts_ref[...], 0, keepdims=True)
    convolutions(nvar, read, total, weights_ref, bias_ref, window, hidden, count, write)


def finish_kernel(nvar, d_ref, base_ref, out_ref, both):
    cols, rows, _ = base_ref.shape
    d = d_ref[...].astype(F32).reshape(cols * rows, LANES)
    left = LANES - nvar
    fine = jnp.where(iota(d.shape, 1) < left, pltpu.roll(d, left, 1), 0.0)
    both[...] = base_ref[...].reshape(cols * rows, LANES) + d + fine
    for r in range(rows):
        turned = both[pl.ds(r, cols, stride=rows), :].T
        out_ref[pl.ds(r, nvar, stride=rows), :] = turned[:nvar]


def exchanged(rows, axes):
    return lax.all_to_all(rows[:, None, :], axes, 0, 0)[:, 0, :]


def body(states, obs_index, obs_values, first_weight, first_bias, second_weight):
    _, nvar, rows, cols = states.shape
    hid = first_weight.shape[0]
    parts = lax.axis_size(TRAJ)
    bands = lax.axis_size(LON)
    count = float(parts * bands * rows * cols)
    each = cols // parts
    vpad = -(-nvar // 8) * 8
    sds = jax.ShapeDtypeStruct
    everyone = sds((parts * bands, LANES), F32)
    band = (cols, rows, LANES)
    source = (states.reshape(nvar * rows, cols), obs_index, obs_values.transpose(1, 0, 2))
    source = [pltpu.with_memory_space_constraint(value, pltpu.HBM) for value in source]
    scratch = [
        pltpu.VMEM((vpad * rows, cols), F32),
        pltpu.VMEM((cols * rows, LANES), F32),
        pltpu.VMEM((LANES, obs_index.shape[1]), F32),
        pltpu.VMEM(obs_index.shape, jnp.int32),
        pltpu.VMEM((nvar, 1, obs_index.shape[1]), F32),
        pltpu.SemaphoreType.DMA((3,)),
    ]
    packed, sums = call(
        functools.partial(prepare_kernel, nvar),
        [sds((cols, 2 * rows, LANES), BF16), sds((bands, LANES), F32)],
        scratch,
        *source,
        far=3,
    )
    wide = 2 * STEPS
    up = [(i, (i + 1) % bands) for i in range(bands)]
    down = [(j, i) for i, j in up]
    left = lax.ppermute(packed[cols - wide :], LON, up)
    right = lax.ppermute(packed[:wide], LON, down)
    (weights,) = call(
        functools.partial(weights_kernel, nvar),
        [sds((2, 9 * hid, hid), BF16)],
        [pltpu.VMEM((hid, hid), F32), pltpu.VMEM(first_weight.shape[::-1], F32)],
        first_weight.T,
        second_weight,
    )
    bias = first_bias[None]
    sent, done = call(
        functools.partial(assemble_kernel, wide),
        [sds((parts, 2 * each + 3 * wide + 1, rows, LANES), BF16), sds((8, LANES), F32)],
        [],
        packed,
        left,
        right,
        exchanged(sums, LON),
    )
    got = lax.all_to_all(sent, TRAJ, 0, 0)
    (base,) = call(functools.partial(base_kernel, nvar), [sds(band, F32)], scratch, *source, done, far=4)
    def buffers(cols):
        return [
            pltpu.VMEM((parts + 2, cols, rows, hid), BF16),
            pltpu.VMEM((parts + 2, cols - 2, rows, hid), BF16),
        ]

    x1, d1, sums1 = call(
        functools.partial(first_step_kernel, nvar, count),
        [sds((parts, each + 4, rows, LANES), F32), sds((parts, each, rows, LANES), F32), everyone],
        buffers(each + 8)
        + [
            pltpu.VMEM((parts, sent.shape[1] - 1, rows, LANES), BF16),
            pltpu.VMEM((parts, rows, LANES), BF16),
            pltpu.SemaphoreType.DMA((parts + 1,)),
        ],
        base,
        pltpu.with_memory_space_constraint(got, pltpu.HBM),
        weights,
        bias,
        far=2,
    )
    (d2,) = call(
        functools.partial(second_step_kernel, nvar, count),
        [sds((parts, each, rows, LANES), BF16)],
        buffers(each + 4),
        x1,
        d1,
        exchanged(sums1, ALL),
        weights,
        bias,
    )
    back = lax.all_to_all(d2, TRAJ, 0, 0)
    (out,) = call(
        functools.partial(finish_kernel, nvar),
        [sds((nvar * rows, cols), F32)],
        [pltpu.VMEM((cols * rows, LANES), F32)],
        back.reshape(cols, rows, LANES),
        base,
    )
    return out.reshape(states.shape)


def solution(mesh):
    torus = Mesh(
        mesh.devices.reshape(4, 2, 2, 4, 2), ("traj_0", "traj_1", "lon_0", "lon_1", "lon_2")
    )
    placed = (P(TRAJ, None, None, LON), P(TRAJ, LON), P(TRAJ, None, LON), P(), P(), P())
    return jax.shard_map(
        body, mesh=torus, in_specs=placed, out_specs=P(TRAJ, None, None, LON), check_vma=False
    )
```
